32 devices in a mesh: gx: 16 (over z, x, core), gy: 2 (over y).
Axes of the slice: x: 2, y: 2, z: 4, core: 2. Of those that a mesh axis runs over, the one named last changes fastest.
Arguments:
- velocity: float32 [256, 256, 512], P('gx', 'gy'), may hold values from -24 to 24
- viscosity: float32 [256], P('gx'), may hold values from 1000 to 8000
- marker_forces: bfloat16 [4096, 16], P(('gx', 'gy')), may hold values from -18 to 18
- spread_weights: bfloat16 [4096, 16, 2048], P(('gx', 'gy')), may hold values from -1.5 to 1.5
- block_owner: int32 [4096, 1], P(('gx', 'gy')), may hold values from 0 to 31; in each aligned block of 128 rows (0 to 127, 128 to 255, ...) at most 8 rows name the same one
- tile_slot: int32 [4096], P(('gx', 'gy')), may hold values from 0 to 511
Outputs:
- relaxed: float32 [256, 256, 512], P('gx', 'gy')
The draws below stay inside these ranges and needn't reach their ends.
Inputs may be any that keep to these rules, and one draw needn't show every extreme that they name: `block_owner`: among the 128 blocks held by one device, no owner is named by more than 8 of them.
All inputs are finite; a program needn't handle non-finite values.
Results may differ from the reference program's by a relative error of at most 0.0013.
Values may be sent and summed in bfloat16 or wider, within the bound.
A program may use at most 128 MiB of HBM per device.

```python
import math
import jax
import jax.numpy as jnp
import numpy as np
from jax import lax

CX = 16
CY = 128
CZ = 512
SEG = 128
MB = 16
BLK_DEV = 128
CAP = 8
TILE = 2048
NX = 256
NY = 256
NZ = 512
NBLK = 4096
N_GX = 16
N_GY = 2
DEVICES = 32


def plant(result, own_key, smallest, top_value):
    longest = result.shape.index(max(result.shape))
    spots = []
    for shift in (0, 1):
        where = [jax.random.randint(jax.random.fold_in(own_key, axis), (), 0, length) for axis, length in enumerate(result.shape)]
        where[longest] = (where[longest] + shift) % result.shape[longest]
        spots.append(tuple(where))
    return result.at[spots[0]].set(smallest).at[spots[1]].set(top_value)


def levels(stream_key, dims, pieces, least, largest):
    gain, own = 1.0, jax.random.fold_in(stream_key, 6)
    for dim, blocks in pieces:
        heights = jnp.exp(jax.random.uniform(jax.random.fold_in(own, dim), (blocks,), jnp.float32, least / len(pieces), largest / len(pieces)))
        gain = gain * jnp.repeat(heights, dims[dim] // blocks).reshape([-1 if axis == dim else 1 for axis in range(len(dims))])
    return gain


def assign_block(rng, own, number, rows, count, top, bound, lean):
    order = jax.random.permutation(rng, count)
    crowded, usual = portions_of(count, rows * top, bound, lean, True), portions_of(count, rows * top, bound, lean, False)
    places = jnp.arange(count)

    def named(tallies, turn):
        used = int((tallies > 0).sum())
        fixed = max(1, used // 4)
        shifted = fixed + (places - fixed + turn * (used - fixed)) % max(1, count - fixed)
        return jnp.zeros((count,), jnp.int32).at[order[jnp.where(places < fixed, places, shifted)]].set(jnp.asarray(tallies, jnp.int32))

    tallies = jnp.where(number % 4 == 0, named(crowded, number // 4), named(usual, number - number // 4 - 1))
    mixed = jax.random.permutation(jax.random.fold_in(own, 3), count)
    donor, sink = mixed[0:count // 2 * 2:2], mixed[1:count // 2 * 2:2]
    margin = jnp.minimum(tallies[donor] - 1, bound - tallies[sink]) // 2
    margin = jnp.where((donor == order[0]) | (sink == order[0]) | (tallies[sink] == 0), 0, jnp.maximum(margin, 0))
    shifted = jax.random.randint(jax.random.fold_in(own, 4), (count // 2,), 0, 1 << 20) % (margin + 1)
    tallies = tallies.at[donor].add(-shifted).at[sink].add(shifted)
    members = jnp.searchsorted(jnp.cumsum(tallies), jnp.arange(rows * top), side="right").astype(jnp.int32)
    grid = members.reshape(top, rows).T
    grid = grid[jax.random.permutation(jax.random.fold_in(own, 1), rows)]
    turn = jax.random.randint(jax.random.fold_in(own, 2), (rows, 1), 0, top)
    return jnp.take_along_axis(grid, (jnp.arange(top)[None, :] + turn) % top, axis=1)


def portions_of(amount, total, bound, slope, full):
    weights = [(1 << 20) // math.isqrt(rank ** slope) + 1 for rank in range(1, amount + 1)]
    largest = bound if full else min(bound, max(-(-total // amount), total * weights[0] // sum(weights)))
    least = 1 if total - largest >= amount - 1 else 0
    counts, surplus = [largest] + [least] * (amount - 1), total - largest - least * (amount - 1)
    while surplus > 0:
        free = [i for i in range(1, amount) if counts[i] < largest] or [i for i in range(1, amount) if counts[i] < bound]
        mass, remaining = sum([weights[i] for i in free]), surplus
        for i in free:
            more = min(bound - counts[i], max(1, remaining * weights[i] // mass), surplus)
            counts[i] = counts[i] + more
            surplus = surplus - more
    return np.array(counts)


def normal_values(own_key, extent, deviation, most, split=(), held_as=jnp.bfloat16):
    array = deviation * jax.random.normal(own_key, extent, jnp.float32)
    if split:
        array = array * levels(own_key, extent, split, -0.22, 0.18)
    return jnp.clip(array, -most, most).astype(held_as)


def setup_inputs(seed: int = 0) -> dict:
    key_of = jax.random.split(jax.random.key(seed), 7)
    velocity = normal_values(key_of[0], (NX, NY, NZ), 4.0, 24.0, ((0, 16), (1, 2)), jnp.float32)
    viscosity = jnp.clip(jnp.exp(math.log(8000.0) - 2.0794415 * jax.random.uniform(key_of[1], (NX,), jnp.float32) ** levels(key_of[1], (NX,), ((0, 16),), -0.2, 0.2)), 1000.0, 8000.0)
    marker_forces = normal_values(key_of[2], (NBLK, MB), 3.0, 18.0, ((0, 32),))
    spread_weights = normal_values(key_of[3], (NBLK, MB, TILE), MB ** -0.5, 1.5, ((0, 32),))
    block_owner_keys = jax.random.split(jax.random.fold_in(key_of[4], 1), NBLK // BLK_DEV)
    block_owner_turns = jax.random.permutation(jax.random.fold_in(key_of[4], 3), NBLK // BLK_DEV)
    block_owner = jax.vmap(lambda own, number: assign_block(jax.random.fold_in(key_of[4], 2), own, number, BLK_DEV, DEVICES, 1, CAP, 2))(block_owner_keys, block_owner_turns).reshape((NBLK, 1))
    tile_slot = plant(jax.random.randint(key_of[5], (NBLK,), 0, CY * (CZ // SEG)), jax.random.fold_in(key_of[5], 1), 0, (CY * (CZ // SEG)) - 1).astype(jnp.int32)
    return {"velocity": velocity, "viscosity": viscosity, "marker_forces": marker_forces, "spread_weights": spread_weights, "block_owner": block_owner, "tile_slot": tile_slot}


def spread_one(pair):
    return jnp.einsum('bm,bmt->bt', pair[0], pair[1].astype(jnp.float32))

def reference(velocity, viscosity, marker_forces, spread_weights, block_owner, tile_slot):
    forces_dev = marker_forces.reshape(DEVICES, BLK_DEV, MB).astype(jnp.float32)
    weights_dev = spread_weights.reshape(DEVICES, BLK_DEV, MB, TILE)
    tile_values = lax.map(spread_one, (forces_dev, weights_dev))
    rounded = lax.optimization_barrier(tile_values.astype(jnp.bfloat16)).astype(jnp.float32)
    rounded = rounded.reshape(NBLK, CX, SEG)
    owner_dev = block_owner[:, 0]
    owner_x = owner_dev // N_GY
    owner_y = owner_dev % N_GY
    row_y = owner_y * CY + tile_slot // (CZ // SEG)
    seg_z = tile_slot % (CZ // SEG)
    force_field = jnp.zeros((N_GX, CX, NY, CZ // SEG, SEG), jnp.float32)
    force_field = force_field.at[owner_x, :, row_y, seg_z, :].add(rounded)
    right_side = velocity.reshape(NX, NY * NZ) + force_field.reshape(NX, NY * NZ)
    below_all = (-viscosity).at[0].set(0.0)
    above_all = (-viscosity).at[NX - 1].set(0.0)
    main_all = 1.0 + 2.0 * viscosity
    solved = lax.linalg.tridiagonal_solve(below_all, main_all, above_all, right_side)
    return solved.reshape(NX, NY, NZ)
```

```python
import functools

import jax
import jax.numpy as jnp
from jax import lax
from jax.experimental import pallas as pl
from jax.experimental.pallas import tpu as pltpu
from jax.sharding import PartitionSpec as P

F32 = jnp.float32
BF16 = jnp.bfloat16
BASE = 256


def iota(shape, axis):
    return lax.broadcasted_iota(jnp.int32, shape, axis)


def nt_dot(a, b):
    return lax.dot_general(a, b, (((1,), (1,)), ((), ())), preferred_element_type=F32)


def spread_kernel(devices, capacity, f_ref, w_ref, owner_ref, slot_ref, out_ref, tiles_ref):
    step = pl.program_id(0)
    group, markers = f_ref.shape
    cells = w_ref.shape[2]
    wide = group * markers
    pick = (iota((markers, wide), 1) % markers == iota((markers, wide), 0)).astype(BF16)
    tiled = jnp.dot(f_ref[...], pick, preferred_element_type=F32)
    block = iota((group, wide), 1) // markers == iota((group, wide), 0)
    forces = jnp.where(block, tiled, 0.0).astype(BF16)
    weights = w_ref[...].reshape(wide, cells)
    tiles = jnp.dot(forces, weights, preferred_element_type=F32).astype(BF16)
    tiles_ref[pl.ds(pl.multiple_of(step * group, group), group), :] = tiles

    @pl.when(step == pl.num_programs(0) - 1)
    def _():
        blocks = owner_ref.shape[1]
        rows = devices * capacity
        owner = owner_ref[...]
        matches = (iota((devices, blocks), 0) == owner).astype(F32)
        earlier = (iota((blocks, blocks), 0) < iota((blocks, blocks), 1)).astype(BF16)
        counts = jnp.dot(matches.astype(BF16), earlier, preferred_element_type=F32)
        rank = jnp.sum(counts * matches, axis=0, keepdims=True).astype(jnp.int32)
        target = owner * capacity + rank
        select = (iota((rows, blocks), 0) == target).astype(BF16)
        out = jnp.dot(select, tiles_ref[...], preferred_element_type=F32)
        number = slot_ref[...] + 1
        lane = iota((128, blocks), 0)
        digits = jnp.where(lane == 0, number // BASE, jnp.where(lane == 1, number % BASE, 0))
        meta = nt_dot(select, digits.astype(F32).astype(BF16))
        if capacity % 8 == 0:
            out_ref[:, :, :cells] = out.reshape(devices, capacity, cells).astype(BF16)
            out_ref[:, :, cells:] = meta.reshape(devices, capacity, 128).astype(BF16)
        else:
            for d in range(devices):
                lo, hi = d * capacity, (d + 1) * capacity
                out_ref[d, :, :cells] = out[lo:hi].astype(BF16)
                out_ref[d, :, cells:] = meta[lo:hi].astype(BF16)


def spread(forces, weights, owner, slots, devices, capacity):
    blocks, markers, cells = weights.shape
    group = min(blocks, max(8, 256 // markers))
    return pl.pallas_call(
        functools.partial(spread_kernel, devices, capacity),
        out_shape=jax.ShapeDtypeStruct((devices, capacity, cells + 128), BF16),
        grid=(blocks // group,),
        in_specs=[
            pl.BlockSpec((group, markers), lambda i: (i, 0)),
            pl.BlockSpec((group, markers, cells), lambda i: (i, 0, 0)),
            pl.BlockSpec((1, blocks), lambda i: (0, 0)),
            pl.BlockSpec((1, blocks), lambda i: (0, 0)),
        ],
        out_specs=pl.BlockSpec((devices, capacity, cells + 128), lambda i: (0, 0, 0)),
        scratch_shapes=[pltpu.VMEM((blocks, cells), BF16)],
        compiler_params=pltpu.CompilerParams(vmem_limit_bytes=24 << 20),
        cost_estimate=pl.CostEstimate(
            flops=2 * blocks * markers * cells * 64, bytes_accessed=weights.size * 2, transcendentals=0
        ),
    )(forces, weights, owner, slots)


def factor(visc):
    inverse, ratio = [], []
    for x in range(len(visc) - 1):
        pivot = 1.0 + 2.0 * visc[x]
        if x:
            pivot = pivot - visc[x] * ratio[-1]
        inverse.append(1.0 / pivot)
        ratio.append(visc[x] * inverse[-1])
    return inverse, ratio


def spikes(inverse, ratio):
    count = len(inverse)
    left = [inverse[0]]
    for x in range(1, count):
        left.append(ratio[x] * left[-1])
    for x in range(count - 2, -1, -1):
        left[x] = left[x] + ratio[x] * left[x + 1]
    right = [inverse[-1]]
    for x in range(count - 2, -1, -1):
        right.append(ratio[x] * right[-1])
    return left, right[::-1]


def local_kernel(visc_ref, velocity_ref, arrived_ref, out_ref, ends_ref, rhs_ref, coef_ref, flat_ref):
    cells_x, rows_y, seg = velocity_ref.shape
    devices, capacity, width = arrived_ref.shape
    rows = devices * capacity
    cells = width - 128
    segments = pl.num_programs(0)
    z = pl.program_id(0)

    @pl.when(z == 0)
    def _():
        visc = [jnp.full((8, seg), visc_ref[x], F32) for x in range(cells_x)]
        inverse, ratio = factor(visc)
        for x in range(cells_x - 1):
            coef_ref[x] = inverse[x]
            coef_ref[cells_x + x] = ratio[x]
        coef_ref[cells_x - 1] = visc[-1]
        if capacity % 8 == 0:
            flat_ref[...] = arrived_ref[...].astype(F32).reshape(rows, width).astype(BF16)
        else:
            parts = [arrived_ref[d].astype(F32) for d in range(devices)]
            flat_ref[...] = jnp.concatenate(parts, axis=0).astype(BF16)

    lane = iota((8, 128), 1)
    base = jnp.where(lane == 0, float(BASE), jnp.where(lane == 1, 1.0, 0.0)).astype(BF16)
    number = nt_dot(base, flat_ref[:, cells:])[0:1, :].astype(jnp.int32) - 1
    place = (iota((rows_y, rows), 0) * segments + z == number).astype(BF16)
    rhs_ref[...] = jnp.dot(place, flat_ref[:, :cells], preferred_element_type=F32)

    def chunk(i, carry):
        at = pl.ds(pl.multiple_of(i * 8, 8), 8)

        def side(x):
            return velocity_ref[x, at, :] + rhs_ref[at, x * seg : (x + 1) * seg]

        values = [side(0) * coef_ref[0]]
        for x in range(1, cells_x - 1):
            values.append(side(x) * coef_ref[x] + coef_ref[cells_x + x] * values[-1])
        last = cells_x - 1
        ends_ref[0, at, :] = side(last) + coef_ref[last] * values[-1]
        value = values[-1]
        out_ref[last - 1, at, :] = value
        for x in range(last - 2, -1, -1):
            value = values[x] + coef_ref[cells_x + x] * value
            out_ref[x, at, :] = value
        ends_ref[1, at, :] = value
        return carry

    lax.fori_loop(0, rows_y // 8, chunk, 0, unroll=2)


def local_solve(viscosity, velocity, arrived, seg):
    cells_x, cells_y, cells_z = velocity.shape
    devices, capacity, width = arrived.shape
    rows = devices * capacity
    return pl.pallas_call(
        local_kernel,
        out_shape=(
            jax.ShapeDtypeStruct((cells_x - 1, cells_y, cells_z), F32),
            jax.ShapeDtypeStruct((2, cells_y, cells_z), F32),
        ),
        grid=(cells_z // seg,),
        in_specs=[
            pl.BlockSpec(memory_space=pltpu.SMEM),
            pl.BlockSpec((cells_x, cells_y, seg), lambda i: (0, 0, i)),
            pl.BlockSpec((devices, capacity, width), lambda i: (0, 0, 0)),
        ],
        out_specs=(
            pl.BlockSpec((cells_x - 1, cells_y, seg), lambda i: (0, 0, i)),
            pl.BlockSpec((2, cells_y, seg), lambda i: (0, 0, i)),
        ),
        scratch_shapes=[
            pltpu.VMEM((cells_y, cells_x * seg), F32),
            pltpu.VMEM((2 * cells_x, 8, seg), F32),
            pltpu.VMEM((rows, width), BF16),
        ],
        compiler_params=pltpu.CompilerParams(vmem_limit_bytes=24 << 20),
    )(viscosity, velocity, arrived)


def couple_kernel(visc_ref, out_ref):
    cells_x, count, lanes = visc_ref.shape
    visc = [visc_ref[x] for x in range(cells_x)]
    inverse, ratio = factor(visc)
    left, right = spikes(inverse, ratio)
    row = iota((count, lanes), 0)

    def following(value):
        moved = jnp.concatenate([value[1:], value[:1]], axis=0)
        return jnp.where(row == count - 1, 0.0, moved)

    sep, inner, first = visc[-1], visc[-2], visc[0]
    lower = jnp.where(row > 0, -sep * first * left[-1], 0.0)
    center = 1.0 + 2.0 * sep - sep * inner * right[-1] - sep * following(first * left[0])
    upper = -sep * following(inner * right[0])
    previous = jnp.zeros((1, lanes), F32)
    for d in range(count):
        pivot = center[d : d + 1] - lower[d : d + 1] * previous
        inv = 1.0 / pivot
        previous = upper[d : d + 1] * inv
        out_ref[0, d : d + 1, :] = inv
        out_ref[1, d : d + 1, :] = previous
    out_ref[2] = lower
    out_ref[3] = jnp.where(row == count - 1, 0.0, sep)


def couple(splat):
    return pl.pallas_call(
        couple_kernel,
        out_shape=jax.ShapeDtypeStruct((4,) + splat.shape[1:], F32),
    )(splat)


def reduced_kernel(coef_ref, sides_ref, out_ref):
    count, rows, cells_z = sides_ref.shape[1:]
    lanes = coef_ref.shape[2]
    for c in range(cells_z // lanes):
        at = slice(c * lanes, (c + 1) * lanes)
        values = []
        for d in range(count):
            side = sides_ref[0, d, :, at]
            if d + 1 < count:
                side = side + coef_ref[3, d : d + 1, :] * sides_ref[1, d + 1, :, at]
            if d:
                side = side - coef_ref[2, d : d + 1, :] * values[-1]
            values.append(side * coef_ref[0, d : d + 1, :])
        value = values[-1]
        out_ref[0, count - 1, :, at] = value
        for d in range(count - 2, -1, -1):
            value = values[d] - coef_ref[1, d : d + 1, :] * value
            out_ref[0, d, :, at] = value
            out_ref[1, d + 1, :, at] = value
        out_ref[1, 0, :, at] = jnp.zeros_like(value)


def reduced(coefs, sides):
    return pl.pallas_call(
        reduced_kernel,
        out_shape=jax.ShapeDtypeStruct(sides.shape, F32),
    )(coefs, sides)


def final_kernel(visc_ref, inner_ref, ends_ref, out_ref, coef_ref):
    count, rows_y, cells_z = inner_ref.shape
    seg = coef_ref.shape[2]

    @pl.when(pl.program_id(0) == 0)
    def _():
        visc = [jnp.full((8, seg), visc_ref[x], F32) for x in range(count + 1)]
        left, right = spikes(*factor(visc))
        for x in range(count):
            coef_ref[x] = visc[0] * left[x]
            coef_ref[count + x] = visc[count - 1] * right[x]

    def chunk(i, carry):
        at = pl.ds(pl.multiple_of(i * 8, 8), 8)
        for c in range(cells_z // seg):
            lane = slice(c * seg, (c + 1) * seg)
            own, before = ends_ref[0, at, lane], ends_ref[1, at, lane]
            for x in range(count):
                out_ref[x, at, lane] = (
                    inner_ref[x, at, lane] + coef_ref[x] * before + coef_ref[count + x] * own
                )
            out_ref[count, at, lane] = own
        return carry

    lax.fori_loop(0, rows_y // 8, chunk, 0)


def final(viscosity, inner, ends, seg):
    count, cells_y, cells_z = inner.shape
    parts = 4
    rows = cells_y // parts
    return pl.pallas_call(
        final_kernel,
        out_shape=jax.ShapeDtypeStruct((count + 1, cells_y, cells_z), F32),
        grid=(parts,),
        in_specs=[
            pl.BlockSpec(memory_space=pltpu.SMEM),
            pl.BlockSpec((count, rows, cells_z), lambda i: (0, i, 0)),
            pl.BlockSpec((2, rows, cells_z), lambda i: (0, i, 0)),
        ],
        out_specs=pl.BlockSpec((count + 1, rows, cells_z), lambda i: (0, i, 0)),
        scratch_shapes=[pltpu.VMEM((2 * count, 8, seg), F32)],
        compiler_params=pltpu.CompilerParams(vmem_limit_bytes=24 << 20),
    )(viscosity, inner, ends)


def per_device(velocity, viscosity, marker_forces, spread_weights, block_owner, tile_slot):
    cells_x, cells_y, cells_z = velocity.shape
    grid_x = lax.axis_size("gx")
    devices = grid_x * lax.axis_size("gy")
    blocks, _, cells = spread_weights.shape
    capacity = max(2, 2 * blocks // devices)
    seg = cells // cells_x
    whole = lax.all_gather(viscosity, "gx", axis=0, tiled=True).reshape(grid_x, cells_x)
    splat = jnp.broadcast_to(whole.T[:, :, None], (cells_x, grid_x, 128))
    outgoing = spread(
        marker_forces,
        spread_weights,
        block_owner.reshape(1, blocks),
        tile_slot.reshape(1, blocks),
        devices,
        capacity,
    )
    arrived = lax.all_to_all(outgoing, ("gx", "gy"), split_axis=0, concat_axis=0, tiled=True)
    coefs = couple(splat)
    inner, ends = local_solve(viscosity, velocity, arrived, seg)
    sides = lax.all_to_all(
        ends.reshape(2, grid_x, -1, cells_z), "gx", split_axis=1, concat_axis=1, tiled=True
    )
    returned = lax.all_to_all(reduced(coefs, sides), "gx", split_axis=1, concat_axis=1, tiled=True)
    return final(viscosity, inner, returned.reshape(2, cells_y, cells_z), seg)


def solution(mesh):
    placed = (
        P("gx", "gy", None),
        P("gx"),
        P(("gx", "gy"), None),
        P(("gx", "gy"), None, None),
        P(("gx", "gy"), None),
        P(("gx", "gy")),
    )
    return jax.shard_map(
        per_device, mesh=mesh, in_specs=placed, out_specs=P("gx", "gy", None), check_vma=False
    )
```

```python
import functools

import jax
import jax.numpy as jnp
from jax import lax
from jax.experimental import pallas as pl
from jax.experimental.pallas import tpu as pltpu
from jax.sharding import PartitionSpec as P

F32 = jnp.float32
BF16 = jnp.bfloat16
BASE = 256


def iota(shape, axis):
    return lax.broadcasted_iota(jnp.int32, shape, axis)


def nt_dot(a, b):
    return lax.dot_general(a, b, (((1,), (1,)), ((), ())), preferred_element_type=F32)


def spread_kernel(
    devices, capacity, visc_ref, f_ref, w_ref, owner_ref, slot_ref, out_ref, splat_ref, tiles_ref
):
    step = pl.program_id(0)
    group, markers = f_ref.shape
    cells = w_ref.shape[2]
    wide = group * markers
    pick = (iota((markers, wide), 1) % markers == iota((markers, wide), 0)).astype(BF16)
    tiled = jnp.dot(f_ref[...], pick, preferred_element_type=F32)
    block = iota((group, wide), 1) // markers == iota((group, wide), 0)
    forces = jnp.where(block, tiled, 0.0).astype(BF16)
    weights = w_ref[...].reshape(wide, cells)
    tiles = jnp.dot(forces, weights, preferred_element_type=F32).astype(BF16)
    tiles_ref[pl.ds(pl.multiple_of(step * group, group), group), :] = tiles

    @pl.when(step == pl.num_programs(0) - 1)
    def _():
        for x in range(splat_ref.shape[0]):
            splat_ref[x : x + 1, :] = jnp.full((1, 128), visc_ref[x], F32)
        blocks = owner_ref.shape[1]
        rows = devices * capacity
        owner = owner_ref[...]
        matches = (iota((devices, blocks), 0) == owner).astype(F32)
        earlier = (iota((blocks, blocks), 0) < iota((blocks, blocks), 1)).astype(BF16)
        counts = jnp.dot(matches.astype(BF16), earlier, preferred_element_type=F32)
        rank = jnp.sum(counts * matches, axis=0, keepdims=True).astype(jnp.int32)
        target = owner * capacity + rank
        select = (iota((rows, blocks), 0) == target).astype(BF16)
        out = jnp.dot(select, tiles_ref[...], preferred_element_type=F32)
        number = slot_ref[...] + 1
        lane = iota((128, blocks), 0)
        digits = jnp.where(lane == 0, number // BASE, jnp.where(lane == 1, number % BASE, 0))
        meta = nt_dot(select, digits.astype(F32).astype(BF16))
        if capacity % 8 == 0:
            out_ref[:, :, :cells] = out.reshape(devices, capacity, cells).astype(BF16)
            out_ref[:, :, cells:] = meta.reshape(devices, capacity, 128).astype(BF16)
        else:
            for d in range(devices):
                lo, hi = d * capacity, (d + 1) * capacity
                out_ref[d, :, :cells] = out[lo:hi].astype(BF16)
                out_ref[d, :, cells:] = meta[lo:hi].astype(BF16)


def spread(viscosity, forces, weights, owner, slots, devices, capacity):
    blocks, markers, cells = weights.shape
    group = min(blocks, max(8, 256 // markers))
    return pl.pallas_call(
        functools.partial(spread_kernel, devices, capacity),
        out_shape=(
            jax.ShapeDtypeStruct((devices, capacity, cells + 128), BF16),
            jax.ShapeDtypeStruct((viscosity.shape[0], 128), F32),
        ),
        grid=(blocks // group,),
        in_specs=[
            pl.BlockSpec(memory_space=pltpu.SMEM),
            pl.BlockSpec((group, markers), lambda i: (i, 0)),
            pl.BlockSpec((group, markers, cells), lambda i: (i, 0, 0)),
            pl.BlockSpec((1, blocks), lambda i: (0, 0)),
            pl.BlockSpec((1, blocks), lambda i: (0, 0)),
        ],
        out_specs=(
            pl.BlockSpec((devices, capacity, cells + 128), lambda i: (0, 0, 0)),
            pl.BlockSpec((viscosity.shape[0], 128), lambda i: (0, 0)),
        ),
        scratch_shapes=[pltpu.VMEM((blocks, cells), BF16)],
        compiler_params=pltpu.CompilerParams(vmem_limit_bytes=24 << 20),
        cost_estimate=pl.CostEstimate(
            flops=2 * blocks * markers * cells * 64, bytes_accessed=weights.size * 2, transcendentals=0
        ),
    )(viscosity, forces, weights, owner, slots)


def factor(visc):
    inverse, ratio = [], []
    for x in range(len(visc) - 1):
        pivot = 1.0 + 2.0 * visc[x]
        if x:
            pivot = pivot - visc[x] * ratio[-1]
        inverse.append(1.0 / pivot)
        ratio.append(visc[x] * inverse[-1])
    return inverse, ratio


def spikes(inverse, ratio):
    count = len(inverse)
    left = [inverse[0]]
    for x in range(1, count):
        left.append(ratio[x] * left[-1])
    for x in range(count - 2, -1, -1):
        left[x] = left[x] + ratio[x] * left[x + 1]
    right = [inverse[-1]]
    for x in range(count - 2, -1, -1):
        right.append(ratio[x] * right[-1])
    return left, right[::-1]


def put(ends_ref, which, i, value):
    rows = ends_ref.shape[2]
    if rows % 8 == 0:
        start = pl.multiple_of(lax.rem(i * 8, rows), 8)
        ends_ref[i * 8 // rows, which, pl.ds(start, 8), :] = value
    else:
        share = 8 // rows
        for k in range(share):
            ends_ref[i * share + k, which] = value[k * rows : (k + 1) * rows]


def get(ends_ref, which, i, lane):
    rows = ends_ref.shape[2]
    if rows % 8 == 0:
        start = pl.multiple_of(lax.rem(i * 8, rows), 8)
        return ends_ref[i * 8 // rows, which, pl.ds(start, 8), lane]
    share = 8 // rows
    return jnp.concatenate([ends_ref[i * share + k, which, :, lane] for k in range(share)], axis=0)


def local_kernel(visc_ref, velocity_ref, arrived_ref, out_ref, ends_ref, rhs_ref, coef_ref, flat_ref):
    cells_x, rows_y, seg = velocity_ref.shape
    devices, capacity, width = arrived_ref.shape
    rows = devices * capacity
    cells = width - 128
    segments = pl.num_programs(0)
    z = pl.program_id(0)

    @pl.when(z == 0)
    def _():
        visc = [jnp.full((8, seg), visc_ref[x], F32) for x in range(cells_x)]
        inverse, ratio = factor(visc)
        for x in range(cells_x - 1):
            coef_ref[x] = inverse[x]
            coef_ref[cells_x + x] = ratio[x]
        coef_ref[cells_x - 1] = visc[-1]
        if capacity % 8 == 0:
            flat_ref[...] = arrived_ref[...].astype(F32).reshape(rows, width).astype(BF16)
        else:
            parts = [arrived_ref[d].astype(F32) for d in range(devices)]
            flat_ref[...] = jnp.concatenate(parts, axis=0).astype(BF16)

    lane = iota((8, 128), 1)
    base = jnp.where(lane == 0, float(BASE), jnp.where(lane == 1, 1.0, 0.0)).astype(BF16)
    number = nt_dot(base, flat_ref[:, cells:])[0:1, :].astype(jnp.int32) - 1
    place = (iota((rows_y, rows), 0) * segments + z == number).astype(BF16)
    rhs_ref[...] = jnp.dot(place, flat_ref[:, :cells], preferred_element_type=F32)

    def chunk(i, carry):
        at = pl.ds(pl.multiple_of(i * 8, 8), 8)

        def side(x):
            return velocity_ref[x, at, :] + rhs_ref[at, x * seg : (x + 1) * seg]

        values = [side(0) * coef_ref[0]]
        for x in range(1, cells_x - 1):
            values.append(side(x) * coef_ref[x] + coef_ref[cells_x + x] * values[-1])
        last = cells_x - 1
        put(ends_ref, 0, i, side(last) + coef_ref[last] * values[-1])
        value = values[-1]
        out_ref[last - 1, at, :] = value
        for x in range(last - 2, -1, -1):
            value = values[x] + coef_ref[cells_x + x] * value
            out_ref[x, at, :] = value
        put(ends_ref, 1, i, value)
        return carry

    lax.fori_loop(0, rows_y // 8, chunk, 0, unroll=2)


def local_solve(viscosity, velocity, arrived, seg, grid_x):
    cells_x, cells_y, cells_z = velocity.shape
    devices, capacity, width = arrived.shape
    rows = devices * capacity
    return pl.pallas_call(
        local_kernel,
        out_shape=(
            jax.ShapeDtypeStruct((cells_x - 1, cells_y, cells_z), F32),
            jax.ShapeDtypeStruct((grid_x, 2, cells_y // grid_x, cells_z), F32),
        ),
        grid=(cells_z // seg,),
        in_specs=[
            pl.BlockSpec(memory_space=pltpu.SMEM),
            pl.BlockSpec((cells_x, cells_y, seg), lambda i: (0, 0, i)),
            pl.BlockSpec((devices, capacity, width), lambda i: (0, 0, 0)),
        ],
        out_specs=(
            pl.BlockSpec((cells_x - 1, cells_y, seg), lambda i: (0, 0, i)),
            pl.BlockSpec((grid_x, 2, cells_y // grid_x, seg), lambda i: (0, 0, 0, i)),
        ),
        scratch_shapes=[
            pltpu.VMEM((cells_y, cells_x * seg), F32),
            pltpu.VMEM((2 * cells_x, 8, seg), F32),
            pltpu.VMEM((rows, width), BF16),
        ],
        compiler_params=pltpu.CompilerParams(vmem_limit_bytes=24 << 20),
    )(viscosity, velocity, arrived)


def couple(visc_ref, out_ref):
    count, cells_x, lanes = visc_ref.shape
    visc = [visc_ref[:, x, :] for x in range(cells_x)]
    inverse, ratio = factor(visc)
    left, right = spikes(inverse, ratio)
    row = iota((count, lanes), 0)

    def following(value):
        moved = jnp.concatenate([value[1:], value[:1]], axis=0)
        return jnp.where(row == count - 1, 0.0, moved)

    sep, inner, first = visc[-1], visc[-2], visc[0]
    lower = jnp.where(row > 0, -sep * first * left[-1], 0.0)
    center = 1.0 + 2.0 * sep - sep * inner * right[-1] - sep * following(first * left[0])
    upper = -sep * following(inner * right[0])
    previous = jnp.zeros((1, lanes), F32)
    for d in range(count):
        pivot = center[d : d + 1] - lower[d : d + 1] * previous
        inv = 1.0 / pivot
        previous = upper[d : d + 1] * inv
        out_ref[0, d : d + 1, :] = inv
        out_ref[1, d : d + 1, :] = previous
    out_ref[2] = lower
    out_ref[3] = jnp.where(row == count - 1, 0.0, sep)


def reduced(coef_ref, sides_ref, out_ref):
    count, _, rows, cells_z = sides_ref.shape
    lanes = coef_ref.shape[2]
    for c in range(cells_z // lanes):
        at = slice(c * lanes, (c + 1) * lanes)
        values = []
        for d in range(count):
            side = sides_ref[d, 0, :, at]
            if d + 1 < count:
                side = side + coef_ref[3, d : d + 1, :] * sides_ref[d + 1, 1, :, at]
            if d:
                side = side - coef_ref[2, d : d + 1, :] * values[-1]
            values.append(side * coef_ref[0, d : d + 1, :])
        value = values[-1]
        out_ref[count - 1, 0, :, at] = value
        for d in range(count - 2, -1, -1):
            value = values[d] - coef_ref[1, d : d + 1, :] * value
            out_ref[d, 0, :, at] = value
            out_ref[d + 1, 1, :, at] = value
        out_ref[0, 1, :, at] = jnp.zeros_like(value)


def greet(count, peer_of):
    barrier = pltpu.get_barrier_semaphore()

    def signal(i, carry):
        pl.semaphore_signal(
            barrier, inc=1, device_id=peer_of(i), device_id_type=pl.DeviceIdType.MESH
        )
        return carry

    lax.fori_loop(1, count, signal, 0)
    pl.semaphore_wait(barrier, count - 1)


def tiles_kernel(count_x, count_y, out_ref, splat_ref, tiles_ref, whole_ref, send, recv, vsend, vrecv, own):
    count = count_x * count_y
    gx, gy = lax.axis_index("gx"), lax.axis_index("gy")
    me = gx * count_y + gy
    half = count // 2

    def peer(i):
        return lax.rem(me + i, count)

    def device(i):
        return (peer(i) // count_y, lax.rem(peer(i), count_y))

    def line_peer(i):
        return (lax.rem(gx + i, count_x), gy)

    def tile_copy(i):
        return pltpu.make_async_remote_copy(
            src_ref=out_ref.at[peer(i)],
            dst_ref=tiles_ref.at[me],
            send_sem=send.at[i],
            recv_sem=recv.at[i],
            device_id=device(i),
            device_id_type=pl.DeviceIdType.MESH,
        )

    def visc_copy(i):
        return pltpu.make_async_remote_copy(
            src_ref=splat_ref,
            dst_ref=whole_ref.at[gx],
            send_sem=vsend.at[i],
            recv_sem=vrecv.at[i],
            device_id=line_peer(i),
            device_id_type=pl.DeviceIdType.MESH,
        )

    own_tile = pltpu.make_async_copy(out_ref.at[me], tiles_ref.at[me], own.at[0])
    own_visc = pltpu.make_async_copy(splat_ref, whole_ref.at[gx], own.at[1])
    own_tile.start()
    own_visc.start()
    greet(count, device)

    def far(i, carry):
        tile_copy(half + i).start()

        @pl.when(i > 0)
        def _():
            tile_copy(i).start()

        return carry

    lax.fori_loop(0, half, far, 0)

    def start_visc(i, carry):
        visc_copy(i).start()
        return carry

    lax.fori_loop(1, count_x, start_visc, 0)

    def finish_tile(i, carry):
        pltpu.make_async_remote_copy(
            src_ref=out_ref.at[peer(i)],
            dst_ref=tiles_ref.at[lax.rem(me + count - i, count)],
            send_sem=send.at[i],
            recv_sem=recv.at[i],
            device_id=device(i),
            device_id_type=pl.DeviceIdType.MESH,
        ).wait()
        return carry

    lax.fori_loop(1, count, finish_tile, 0)

    def finish_visc(i, carry):
        pltpu.make_async_remote_copy(
            src_ref=splat_ref,
            dst_ref=whole_ref.at[lax.rem(gx + count_x - i, count_x)],
            send_sem=vsend.at[i],
            recv_sem=vrecv.at[i],
            device_id=line_peer(i),
            device_id_type=pl.DeviceIdType.MESH,
        ).wait()
        return carry

    lax.fori_loop(1, count_x, finish_visc, 0)
    own_tile.wait()
    own_visc.wait()


def exchange_tiles(outgoing, splat, count_x, count_y):
    anywhere = pl.BlockSpec(memory_space=pl.ANY)
    dma = pltpu.SemaphoreType.DMA
    return pl.pallas_call(
        functools.partial(tiles_kernel, count_x, count_y),
        out_shape=(
            jax.ShapeDtypeStruct(outgoing.shape, BF16),
            jax.ShapeDtypeStruct((count_x,) + splat.shape, F32),
        ),
        in_specs=[anywhere, anywhere],
        out_specs=(anywhere, anywhere),
        scratch_shapes=[
            dma((count_x * count_y,)),
            dma((count_x * count_y,)),
            dma((count_x,)),
            dma((count_x,)),
            dma((2,)),
        ],
        compiler_params=pltpu.CompilerParams(
            collective_id=0, has_side_effects=True, vmem_limit_bytes=16 << 20
        ),
    )(outgoing, splat)


def lines_kernel(
    count, ends_ref, whole_ref, out_ref, sides_ref, solved_ref, coef_ref, send, recv, back, home, own
):
    gx, gy = lax.axis_index("gx"), lax.axis_index("gy")

    def peer(i):
        return lax.rem(gx + i, count)

    def device(i):
        return (peer(i), gy)

    def copy(source, target, slot, sends, receives, i):
        return pltpu.make_async_remote_copy(
            src_ref=source.at[peer(i)],
            dst_ref=target.at[slot],
            send_sem=sends.at[i],
            recv_sem=receives.at[i],
            device_id=device(i),
            device_id_type=pl.DeviceIdType.MESH,
        )

    def start_all(source, target, sends, receives):
        half = count // 2

        def start(i, carry):
            copy(source, target, gx, sends, receives, half + i).start()

            @pl.when(i > 0)
            def _():
                copy(source, target, gx, sends, receives, i).start()

            return carry

        lax.fori_loop(0, half, start, 0)

    def finish_all(source, target, sends, receives):
        def finish(i, carry):
            copy(source, target, lax.rem(gx + count - i, count), sends, receives, i).wait()
            return carry

        lax.fori_loop(1, count, finish, 0)

    greet(count, device)
    start_all(ends_ref, sides_ref, send, recv)
    mine = pltpu.make_async_copy(ends_ref.at[gx], sides_ref.at[gx], own.at[0])
    mine.start()
    couple(whole_ref, coef_ref)
    mine.wait()
    finish_all(ends_ref, sides_ref, send, recv)
    reduced(coef_ref, sides_ref, solved_ref)
    kept = pltpu.make_async_copy(solved_ref.at[gx], out_ref.at[gx], own.at[1])
    kept.start()
    start_all(solved_ref, out_ref, back, home)
    kept.wait()
    finish_all(solved_ref, out_ref, back, home)


def exchange_lines(ends, whole):
    count = ends.shape[0]
    dma = pltpu.SemaphoreType.DMA
    return pl.pallas_call(
        functools.partial(lines_kernel, count),
        out_shape=jax.ShapeDtypeStruct(ends.shape, F32),
        in_specs=[pl.BlockSpec(memory_space=pltpu.VMEM)] * 2,
        out_specs=pl.BlockSpec(memory_space=pltpu.VMEM),
        scratch_shapes=[
            pltpu.VMEM(ends.shape, F32),
            pltpu.VMEM(ends.shape, F32),
            pltpu.VMEM((4, count, 128), F32),
            dma((count,)),
            dma((count,)),
            dma((count,)),
            dma((count,)),
            dma((2,)),
        ],
        compiler_params=pltpu.CompilerParams(
            collective_id=1, has_side_effects=True, vmem_limit_bytes=16 << 20
        ),
    )(ends, whole)


def final_kernel(visc_ref, inner_ref, ends_ref, out_ref, coef_ref):
    count, rows_y, cells_z = inner_ref.shape
    seg = coef_ref.shape[2]

    @pl.when(pl.program_id(0) == 0)
    def _():
        visc = [jnp.full((8, seg), visc_ref[x], F32) for x in range(count + 1)]
        left, right = spikes(*factor(visc))
        for x in range(count):
            coef_ref[x] = visc[0] * left[x]
            coef_ref[count + x] = visc[count - 1] * right[x]

    def chunk(i, carry):
        at = pl.ds(pl.multiple_of(i * 8, 8), 8)
        for c in range(cells_z // seg):
            lane = slice(c * seg, (c + 1) * seg)
            own, before = get(ends_ref, 0, i, lane), get(ends_ref, 1, i, lane)
            for x in range(count):
                out_ref[x, at, lane] = (
                    inner_ref[x, at, lane] + coef_ref[x] * before + coef_ref[count + x] * own
                )
            out_ref[count, at, lane] = own
        return carry

    lax.fori_loop(0, rows_y // 8, chunk, 0)


def final(viscosity, inner, ends, seg):
    count, cells_y, cells_z = inner.shape
    parts = 4
    rows = cells_y // parts
    return pl.pallas_call(
        final_kernel,
        out_shape=jax.ShapeDtypeStruct((count + 1, cells_y, cells_z), F32),
        grid=(parts,),
        in_specs=[
            pl.BlockSpec(memory_space=pltpu.SMEM),
            pl.BlockSpec((count, rows, cells_z), lambda i: (0, i, 0)),
            pl.BlockSpec((ends.shape[0] // parts,) + ends.shape[1:], lambda i: (i, 0, 0, 0)),
        ],
        out_specs=pl.BlockSpec((count + 1, rows, cells_z), lambda i: (0, i, 0)),
        scratch_shapes=[pltpu.VMEM((2 * count, 8, seg), F32)],
        compiler_params=pltpu.CompilerParams(vmem_limit_bytes=24 << 20),
    )(viscosity, inner, ends)


def per_device(velocity, viscosity, marker_forces, spread_weights, block_owner, tile_slot):
    cells_x, cells_y, cells_z = velocity.shape
    grid_x = lax.axis_size("gx")
    devices = grid_x * lax.axis_size("gy")
    blocks, _, cells = spread_weights.shape
    capacity = max(2, 2 * blocks // devices)
    seg = cells // cells_x
    outgoing, splat = spread(
        viscosity,
        marker_forces,
        spread_weights,
        block_owner.reshape(1, blocks),
        tile_slot.reshape(1, blocks),
        devices,
        capacity,
    )
    arrived, whole = exchange_tiles(outgoing, splat, grid_x, devices // grid_x)
    inner, ends = local_solve(viscosity, velocity, arrived, seg, grid_x)
    returned = exchange_lines(ends, whole)
    return final(viscosity, inner, returned, seg)


def solution(mesh):
    placed = (
        P("gx", "gy", None),
        P("gx"),
        P(("gx", "gy"), None),
        P(("gx", "gy"), None, None),
        P(("gx", "gy"), None),
        P(("gx", "gy")),
    )
    return jax.shard_map(
        per_device, mesh=mesh, in_specs=placed, out_specs=P("gx", "gy", None), check_vma=False
    )
```

```python
import functools

import jax
import jax.numpy as jnp
from jax import lax
from jax.experimental import pallas as pl
from jax.experimental.pallas import tpu as pltpu
from jax.sharding import PartitionSpec as P

F32 = jnp.float32
BF16 = jnp.bfloat16
BASE = 256


def iota(shape, axis):
    return lax.broadcasted_iota(jnp.int32, shape, axis)


def nt_dot(a, b):
    return lax.dot_general(a, b, (((1,), (1,)), ((), ())), preferred_element_type=F32)


def spread_kernel(
    devices, capacity, visc_ref, f_ref, w_ref, owner_ref, slot_ref, out_ref, splat_ref, tiles_ref
):
    step = pl.program_id(0)
    group, markers = f_ref.shape
    cells = w_ref.shape[2]
    wide = group * markers
    pick = (iota((markers, wide), 1) % markers == iota((markers, wide), 0)).astype(BF16)
    tiled = jnp.dot(f_ref[...], pick, preferred_element_type=F32)
    block = iota((group, wide), 1) // markers == iota((group, wide), 0)
    forces = jnp.where(block, tiled, 0.0).astype(BF16)
    weights = w_ref[...].reshape(wide, cells)
    tiles = jnp.dot(forces, weights, preferred_element_type=F32).astype(BF16)
    tiles_ref[pl.ds(pl.multiple_of(step * group, group), group), :] = tiles

    @pl.when(step == pl.num_programs(0) - 1)
    def _():
        for x in range(splat_ref.shape[0]):
            splat_ref[x : x + 1, :] = jnp.full((1, 128), visc_ref[x], F32)
        blocks = owner_ref.shape[1]
        rows = devices * capacity
        owner = owner_ref[...]
        matches = (iota((devices, blocks), 0) == owner).astype(F32)
        earlier = (iota((blocks, blocks), 0) < iota((blocks, blocks), 1)).astype(BF16)
        counts = jnp.dot(matches.astype(BF16), earlier, preferred_element_type=F32)
        rank = jnp.sum(counts * matches, axis=0, keepdims=True).astype(jnp.int32)
        target = owner * capacity + rank
        select = (iota((rows, blocks), 0) == target).astype(BF16)
        out = jnp.dot(select, tiles_ref[...], preferred_element_type=F32)
        number = slot_ref[...] + 1
        lane = iota((128, blocks), 0)
        digits = jnp.where(lane == 0, number // BASE, jnp.where(lane == 1, number % BASE, 0))
        meta = nt_dot(select, digits.astype(F32).astype(BF16))
        if capacity % 8 == 0:
            out_ref[:, :, :cells] = out.reshape(devices, capacity, cells).astype(BF16)
            out_ref[:, :, cells:] = meta.reshape(devices, capacity, 128).astype(BF16)
        else:
            for d in range(devices):
                lo, hi = d * capacity, (d + 1) * capacity
                out_ref[d, :, :cells] = out[lo:hi].astype(BF16)
                out_ref[d, :, cells:] = meta[lo:hi].astype(BF16)


def spread(viscosity, forces, weights, owner, slots, devices, capacity):
    blocks, markers, cells = weights.shape
    group = min(blocks, max(8, 256 // markers))
    return pl.pallas_call(
        functools.partial(spread_kernel, devices, capacity),
        out_shape=(
            jax.ShapeDtypeStruct((devices, capacity, cells + 128), BF16),
            jax.ShapeDtypeStruct((viscosity.shape[0], 128), F32),
        ),
        grid=(blocks // group,),
        in_specs=[
            pl.BlockSpec(memory_space=pltpu.SMEM),
            pl.BlockSpec((group, markers), lambda i: (i, 0)),
            pl.BlockSpec((group, markers, cells), lambda i: (i, 0, 0)),
            pl.BlockSpec((1, blocks), lambda i: (0, 0)),
            pl.BlockSpec((1, blocks), lambda i: (0, 0)),
        ],
        out_specs=(
            pl.BlockSpec((devices, capacity, cells + 128), lambda i: (0, 0, 0)),
            pl.BlockSpec((viscosity.shape[0], 128), lambda i: (0, 0)),
        ),
        scratch_shapes=[pltpu.VMEM((blocks, cells), BF16)],
        compiler_params=pltpu.CompilerParams(vmem_limit_bytes=24 << 20),
        cost_estimate=pl.CostEstimate(
            flops=2 * blocks * markers * cells * 64, bytes_accessed=weights.size * 2, transcendentals=0
        ),
    )(viscosity, forces, weights, owner, slots)


def factor(visc):
    inverse, ratio = [], []
    for x in range(len(visc) - 1):
        pivot = 1.0 + 2.0 * visc[x]
        if x:
            pivot = pivot - visc[x] * ratio[-1]
        inverse.append(1.0 / pivot)
        ratio.append(visc[x] * inverse[-1])
    return inverse, ratio


def spikes(inverse, ratio):
    count = len(inverse)
    left = [inverse[0]]
    for x in range(1, count):
        left.append(ratio[x] * left[-1])
    for x in range(count - 2, -1, -1):
        left[x] = left[x] + ratio[x] * left[x + 1]
    right = [inverse[-1]]
    for x in range(count - 2, -1, -1):
        right.append(ratio[x] * right[-1])
    return left, right[::-1]


def put(ends_ref, which, i, value):
    rows = ends_ref.shape[2]
    if rows % 8 == 0:
        start = pl.multiple_of(lax.rem(i * 8, rows), 8)
        ends_ref[i * 8 // rows, which, pl.ds(start, 8), :] = value
    else:
        share = 8 // rows
        for k in range(share):
            ends_ref[i * share + k, which] = value[k * rows : (k + 1) * rows]


def get(ref, i, lane):
    rows = ref.shape[1]
    if rows % 8 == 0:
        start = pl.multiple_of(lax.rem(i * 8, rows), 8)
        return ref[i * 8 // rows, pl.ds(start, 8), lane].astype(F32)
    share = 8 // rows
    parts = [ref[i * share + k, :, lane].astype(F32) for k in range(share)]
    return jnp.concatenate(parts, axis=0)


def local_kernel(visc_ref, velocity_ref, arrived_ref, out_ref, ends_ref, rhs_ref, coef_ref, flat_ref):
    cells_x, rows_y, seg = velocity_ref.shape
    devices, capacity, width = arrived_ref.shape
    rows = devices * capacity
    cells = width - 128
    segments = pl.num_programs(0)
    z = pl.program_id(0)

    @pl.when(z == 0)
    def _():
        visc = [jnp.full((8, seg), visc_ref[x], F32) for x in range(cells_x)]
        inverse, ratio = factor(visc)
        for x in range(cells_x - 1):
            coef_ref[x] = inverse[x]
            coef_ref[cells_x + x] = ratio[x]
        coef_ref[cells_x - 1] = visc[-1]
        if capacity % 8 == 0:
            flat_ref[...] = arrived_ref[...].astype(F32).reshape(rows, width).astype(BF16)
        else:
            parts = [arrived_ref[d].astype(F32) for d in range(devices)]
            flat_ref[...] = jnp.concatenate(parts, axis=0).astype(BF16)

    lane = iota((8, 128), 1)
    base = jnp.where(lane == 0, float(BASE), jnp.where(lane == 1, 1.0, 0.0)).astype(BF16)
    number = nt_dot(base, flat_ref[:, cells:])[0:1, :].astype(jnp.int32) - 1
    place = (iota((rows_y, rows), 0) * segments + z == number).astype(BF16)
    rhs_ref[...] = jnp.dot(place, flat_ref[:, :cells], preferred_element_type=F32)

    def chunk(i, carry):
        at = pl.ds(pl.multiple_of(i * 8, 8), 8)

        def side(x):
            return velocity_ref[x, at, :] + rhs_ref[at, x * seg : (x + 1) * seg]

        values = [side(0) * coef_ref[0]]
        for x in range(1, cells_x - 1):
            values.append(side(x) * coef_ref[x] + coef_ref[cells_x + x] * values[-1])
        last = cells_x - 1
        put(ends_ref, 0, i, side(last) + coef_ref[last] * values[-1])
        value = values[-1]
        out_ref[last - 1, at, :] = value
        for x in range(last - 2, -1, -1):
            value = values[x] + coef_ref[cells_x + x] * value
            out_ref[x, at, :] = value
        put(ends_ref, 1, i, value)
        return carry

    lax.fori_loop(0, rows_y // 8, chunk, 0, unroll=2)


def local_solve(viscosity, velocity, arrived, seg, grid_x):
    cells_x, cells_y, cells_z = velocity.shape
    devices, capacity, width = arrived.shape
    rows = devices * capacity
    return pl.pallas_call(
        local_kernel,
        out_shape=(
            jax.ShapeDtypeStruct((cells_x - 1, cells_y, cells_z), F32),
            jax.ShapeDtypeStruct((grid_x, 2, cells_y // grid_x, cells_z), F32),
        ),
        grid=(cells_z // seg,),
        in_specs=[
            pl.BlockSpec(memory_space=pltpu.SMEM),
            pl.BlockSpec((cells_x, cells_y, seg), lambda i: (0, 0, i)),
            pl.BlockSpec((devices, capacity, width), lambda i: (0, 0, 0)),
        ],
        out_specs=(
            pl.BlockSpec((cells_x - 1, cells_y, seg), lambda i: (0, 0, i)),
            pl.BlockSpec((grid_x, 2, cells_y // grid_x, seg), lambda i: (0, 0, 0, i)),
        ),
        scratch_shapes=[
            pltpu.VMEM((cells_y, cells_x * seg), F32),
            pltpu.VMEM((2 * cells_x, 8, seg), F32),
            pltpu.VMEM((rows, width), BF16),
        ],
        compiler_params=pltpu.CompilerParams(vmem_limit_bytes=24 << 20),
    )(viscosity, velocity, arrived)


def couple(visc_ref, out_ref):
    count, cells_x, lanes = visc_ref.shape
    visc = [visc_ref[:, x, :] for x in range(cells_x)]
    inverse, ratio = factor(visc)
    left, right = spikes(inverse, ratio)
    row = iota((count, lanes), 0)

    def following(value):
        moved = jnp.concatenate([value[1:], value[:1]], axis=0)
        return jnp.where(row == count - 1, 0.0, moved)

    sep, inner, first = visc[-1], visc[-2], visc[0]
    lower = jnp.where(row > 0, -sep * first * left[-1], 0.0)
    center = 1.0 + 2.0 * sep - sep * inner * right[-1] - sep * following(first * left[0])
    upper = -sep * following(inner * right[0])
    previous = jnp.zeros((1, lanes), F32)
    for d in range(count):
        pivot = center[d : d + 1] - lower[d : d + 1] * previous
        inv = 1.0 / pivot
        previous = upper[d : d + 1] * inv
        out_ref[0, d : d + 1, :] = inv
        out_ref[1, d : d + 1, :] = previous
    out_ref[2] = lower
    out_ref[3] = jnp.where(row == count - 1, 0.0, sep)


def reduced(coef_ref, sides_ref, out_ref, step_ref):
    count, _, rows, cells_z = sides_ref.shape
    lanes = coef_ref.shape[2]
    for c in range(cells_z // lanes):
        at = slice(c * lanes, (c + 1) * lanes)
        values = []
        for d in range(count):
            side = sides_ref[d, 0, :, at]
            if d + 1 < count:
                side = side + coef_ref[3, d : d + 1, :] * sides_ref[d + 1, 1, :, at]
            if d:
                side = side - coef_ref[2, d : d + 1, :] * values[-1]
            values.append(side * coef_ref[0, d : d + 1, :])
        value = values[-1]
        out_ref[count - 1, :, at] = value
        for d in range(count - 2, -1, -1):
            before = values[d] - coef_ref[1, d : d + 1, :] * value
            out_ref[d, :, at] = before
            step_ref[d + 1, :, at] = (before - value).astype(BF16)
            value = before
        step_ref[0, :, at] = (-value).astype(BF16)


def partner(me, k, count, sign=1):
    if count & (count - 1):
        return lax.rem(me + count + sign * k, count)
    total, bit = 0, 1
    while bit < count:
        total = total + bit * lax.rem(lax.rem(me // bit, 2) + lax.rem(k // bit, 2), 2)
        bit *= 2
    return total


def greet(count, peer_of):
    barrier = pltpu.get_barrier_semaphore()

    def signal(i, carry):
        pl.semaphore_signal(
            barrier, inc=1, device_id=peer_of(i), device_id_type=pl.DeviceIdType.MESH
        )
        return carry

    lax.fori_loop(1, count, signal, 0)
    pl.semaphore_wait(barrier, count - 1)


def tiles_kernel(count_x, count_y, out_ref, splat_ref, tiles_ref, whole_ref, send, recv, vsend, vrecv, own):
    count = count_x * count_y
    gx, gy = lax.axis_index("gx"), lax.axis_index("gy")
    me = gx * count_y + gy

    def device(i):
        peer = partner(me, i, count)
        return (peer // count_y, lax.rem(peer, count_y))

    def tile_copy(i, slot):
        peer = partner(me, i, count)
        return pltpu.make_async_remote_copy(
            src_ref=out_ref.at[peer],
            dst_ref=tiles_ref.at[slot],
            send_sem=send.at[i],
            recv_sem=recv.at[i],
            device_id=(peer // count_y, lax.rem(peer, count_y)),
            device_id_type=pl.DeviceIdType.MESH,
        )

    def visc_copy(i, slot):
        return pltpu.make_async_remote_copy(
            src_ref=splat_ref,
            dst_ref=whole_ref.at[slot],
            send_sem=vsend.at[i],
            recv_sem=vrecv.at[i],
            device_id=(partner(gx, i, count_x), gy),
            device_id_type=pl.DeviceIdType.MESH,
        )

    own_tile = pltpu.make_async_copy(out_ref.at[me], tiles_ref.at[me], own.at[0])
    own_visc = pltpu.make_async_copy(splat_ref, whole_ref.at[gx], own.at[1])
    own_tile.start()
    own_visc.start()
    greet(count, device)

    def start_tile(i, carry):
        tile_copy(i, me).start()
        return carry

    def start_visc(i, carry):
        visc_copy(i, gx).start()
        return carry

    def finish_tile(i, carry):
        tile_copy(i, partner(me, i, count, -1)).wait()
        return carry

    def finish_visc(i, carry):
        visc_copy(i, partner(gx, i, count_x, -1)).wait()
        return carry

    lax.fori_loop(1, count, start_tile, 0)
    lax.fori_loop(1, count_x, start_visc, 0)
    lax.fori_loop(1, count, finish_tile, 0)
    lax.fori_loop(1, count_x, finish_visc, 0)
    own_tile.wait()
    own_visc.wait()


def exchange_tiles(outgoing, splat, count_x, count_y):
    anywhere = pl.BlockSpec(memory_space=pl.ANY)
    dma = pltpu.SemaphoreType.DMA
    return pl.pallas_call(
        functools.partial(tiles_kernel, count_x, count_y),
        out_shape=(
            jax.ShapeDtypeStruct(outgoing.shape, BF16),
            jax.ShapeDtypeStruct((count_x,) + splat.shape, F32),
        ),
        in_specs=[anywhere, anywhere],
        out_specs=(anywhere, anywhere),
        scratch_shapes=[
            dma((count_x * count_y,)),
            dma((count_x * count_y,)),
            dma((count_x,)),
            dma((count_x,)),
            dma((2,)),
        ],
        compiler_params=pltpu.CompilerParams(
            collective_id=0, has_side_effects=True, vmem_limit_bytes=16 << 20
        ),
    )(outgoing, splat)


def lines_kernel(
    count, ends_ref, whole_ref, out_ref, step_ref,
    sides_ref, solved_ref, steps_ref, coef_ref, send, recv, back, home, back_step, home_step, own
):
    gx, gy = lax.axis_index("gx"), lax.axis_index("gy")

    def device(i):
        return (partner(gx, i, count), gy)

    def copy(source, target, slot, sends, receives, i):
        peer = partner(gx, i, count)
        return pltpu.make_async_remote_copy(
            src_ref=source.at[peer],
            dst_ref=target.at[slot],
            send_sem=sends.at[i],
            recv_sem=receives.at[i],
            device_id=(peer, gy),
            device_id_type=pl.DeviceIdType.MESH,
        )

    def start_all(*groups):
        def start(i, carry):
            for source, target, sends, receives in groups:
                copy(source, target, gx, sends, receives, i).start()
            return carry

        lax.fori_loop(1, count, start, 0)

    def finish_all(*groups):
        def finish(i, carry):
            for source, target, sends, receives in groups:
                copy(source, target, partner(gx, i, count, -1), sends, receives, i).wait()
            return carry

        lax.fori_loop(1, count, finish, 0)

    outward = (ends_ref, sides_ref, send, recv)
    homeward = (
        (solved_ref, out_ref, back, home),
        (steps_ref, step_ref, back_step, home_step),
    )
    greet(count, device)
    start_all(outward)
    mine = pltpu.make_async_copy(ends_ref.at[gx], sides_ref.at[gx], own.at[0])
    mine.start()
    couple(whole_ref, coef_ref)
    mine.wait()
    finish_all(outward)
    reduced(coef_ref, sides_ref, solved_ref, steps_ref)
    kept = pltpu.make_async_copy(solved_ref.at[gx], out_ref.at[gx], own.at[1])
    kept_step = pltpu.make_async_copy(steps_ref.at[gx], step_ref.at[gx], own.at[2])
    kept.start()
    kept_step.start()
    start_all(*homeward)
    kept.wait()
    kept_step.wait()
    finish_all(*homeward)


def exchange_lines(ends, whole):
    count = ends.shape[0]
    single = (count,) + ends.shape[2:]
    dma = pltpu.SemaphoreType.DMA
    return pl.pallas_call(
        functools.partial(lines_kernel, count),
        out_shape=(jax.ShapeDtypeStruct(single, F32), jax.ShapeDtypeStruct(single, BF16)),
        in_specs=[pl.BlockSpec(memory_space=pltpu.VMEM)] * 2,
        out_specs=(pl.BlockSpec(memory_space=pltpu.VMEM),) * 2,
        scratch_shapes=[
            pltpu.VMEM(ends.shape, F32),
            pltpu.VMEM(single, F32),
            pltpu.VMEM(single, BF16),
            pltpu.VMEM((4, count, 128), F32),
            dma((count,)),
            dma((count,)),
            dma((count,)),
            dma((count,)),
            dma((count,)),
            dma((count,)),
            dma((3,)),
        ],
        compiler_params=pltpu.CompilerParams(
            collective_id=1, has_side_effects=True, vmem_limit_bytes=16 << 20
        ),
    )(ends, whole)


def final_kernel(visc_ref, inner_ref, own_ref, step_ref, out_ref, coef_ref):
    count, rows_y, cells_z = inner_ref.shape
    seg = coef_ref.shape[2]

    @pl.when(pl.program_id(0) == 0)
    def _():
        visc = [jnp.full((8, seg), visc_ref[x], F32) for x in range(count + 1)]
        left, right = spikes(*factor(visc))
        for x in range(count):
            coef_ref[x] = visc[0] * left[x]
            coef_ref[count + x] = visc[count - 1] * right[x]

    def chunk(i, carry):
        at = pl.ds(pl.multiple_of(i * 8, 8), 8)
        for c in range(cells_z // seg):
            lane = slice(c * seg, (c + 1) * seg)
            own = get(own_ref, i, lane)
            before = own + get(step_ref, i, lane)
            for x in range(count):
                out_ref[x, at, lane] = (
                    inner_ref[x, at, lane] + coef_ref[x] * before + coef_ref[count + x] * own
                )
            out_ref[count, at, lane] = own
        return carry

    lax.fori_loop(0, rows_y // 8, chunk, 0)


def final(viscosity, inner, own, step, seg):
    count, cells_y, cells_z = inner.shape
    parts = 4
    rows = cells_y // parts
    return pl.pallas_call(
        final_kernel,
        out_shape=jax.ShapeDtypeStruct((count + 1, cells_y, cells_z), F32),
        grid=(parts,),
        in_specs=[
            pl.BlockSpec(memory_space=pltpu.SMEM),
            pl.BlockSpec((count, rows, cells_z), lambda i: (0, i, 0)),
            pl.BlockSpec((own.shape[0] // parts,) + own.shape[1:], lambda i: (i, 0, 0)),
            pl.BlockSpec((own.shape[0] // parts,) + own.shape[1:], lambda i: (i, 0, 0)),
        ],
        out_specs=pl.BlockSpec((count + 1, rows, cells_z), lambda i: (0, i, 0)),
        scratch_shapes=[pltpu.VMEM((2 * count, 8, seg), F32)],
        compiler_params=pltpu.CompilerParams(vmem_limit_bytes=24 << 20),
    )(viscosity, inner, own, step)


def per_device(velocity, viscosity, marker_forces, spread_weights, block_owner, tile_slot):
    cells_x, cells_y, cells_z = velocity.shape
    grid_x = lax.axis_size("gx")
    devices = grid_x * lax.axis_size("gy")
    blocks, _, cells = spread_weights.shape
    capacity = max(2, 2 * blocks // devices)
    seg = cells // cells_x
    outgoing, splat = spread(
        viscosity,
        marker_forces,
        pltpu.with_memory_space_constraint(spread_weights, pltpu.HBM),
        block_owner.reshape(1, blocks),
        tile_slot.reshape(1, blocks),
        devices,
        capacity,
    )
    arrived, whole = exchange_tiles(outgoing, splat, grid_x, devices // grid_x)
    inner, ends = local_solve(viscosity, velocity, arrived, seg, grid_x)
    own, step = exchange_lines(ends, whole)
    return final(viscosity, inner, own, step, seg)


def solution(mesh):
    placed = (
        P("gx", "gy", None),
        P("gx"),
        P(("gx", "gy"), None),
        P(("gx", "gy"), None, None),
        P(("gx", "gy"), None),
        P(("gx", "gy")),
    )
    return jax.shard_map(
        per_device, mesh=mesh, in_specs=placed, out_specs=P("gx", "gy", None), check_vma=False
    )
```
